128 devices in a mesh: node: 8 (over z, core), local: 16 (over y, x).
Axes of the slice: x: 4, y: 4, z: 4, core: 2. Of those that a mesh axis runs over, the one named last changes fastest.
Arguments:
- tokens: bfloat16 [2048, 7168], P(('node', 'local')), may hold values from -6 to 6
- grad_out: bfloat16 [2048, 7168], P(('node', 'local')), may hold values from -6 to 6
- gates: bfloat16 [2048, 3], P(('node', 'local')), may hold values from 0.19921875 to 1
- expert_ids: int32 [2048, 3], P(('node', 'local')), may hold values from 0 to 15, as said below
- w_gate: bfloat16 [8, 7168, 2048], P('node', None, 'local'), may hold values from -0.0625 to 0.0625
- w_up: bfloat16 [8, 7168, 2048], P('node', None, 'local'), may hold values from -0.0625 to 0.0625
- w_down: bfloat16 [8, 7168, 2048], P('node', None, 'local'), may hold values from -0.1875 to 0.1875
- s_gate: bfloat16 [7168, 2048], P(None, 'local'), may hold values from -0.0625 to 0.0625
- s_up: bfloat16 [7168, 2048], P(None, 'local'), may hold values from -0.0625 to 0.0625
- s_down: bfloat16 [7168, 2048], P(None, 'local'), may hold values from -0.125 to 0.125
Outputs:
- dx: bfloat16 [2048, 7168], P(('node', 'local'))
- dgates: float32 [2048, 3], P(('node', 'local'))
- d_w_gate: bfloat16 [8, 7168, 2048], P('node', None, 'local')
- d_w_up: bfloat16 [8, 7168, 2048], P('node', None, 'local')
- d_w_down: bfloat16 [8, 7168, 2048], P('node', None, 'local')
- d_s_gate: bfloat16 [7168, 2048], P('node', 'local')
- d_s_up: bfloat16 [7168, 2048], P('node', 'local')
- d_s_down: bfloat16 [7168, 2048], P('node', 'local')
The draws below stay inside these ranges and needn't reach their ends.
Inputs may be any that keep to these rules, and one draw needn't show every extreme that they name: `expert_ids`: each token names both experts of one node and one expert of a second node. Of the tokens of one device exactly 4 name experts of each node and at most 4 name any one expert; for every node one of its experts is named by exactly 4 tokens of every device.
All inputs are finite; a program needn't handle non-finite values.
Results may differ from the reference program's by a relative error of at most 0.014.
Values may be sent and summed in bfloat16 or wider, within the bound.
No kernel may reach another device: no remote copies, remote signals or barrier semaphores. Data moves between devices by JAX's collectives and lax.ppermute only.
A program may use at most 192 MiB of HBM per device.

```python
import jax
import jax.numpy as jnp
from jax import lax

D = 7168
FF = 1024
FFS = 2048
TOPK = 3
E_NODE = 2
TOK_DEV = 16
TOKENS = 2048
EXPERTS = 16
N_NODE = 8
N_LOCAL = 16


def draw_expert_ids(key, part):
    node_count = EXPERTS // E_NODE
    device_count = TOKENS // TOK_DEV
    keys = jax.random.split(key, 4)
    node_order = jax.vmap(lambda item: jax.random.permutation(item, node_count))(jax.random.split(keys[0], device_count))
    position = jnp.arange(TOK_DEV, dtype=jnp.int32)
    first_slot = position % node_count
    second_slot = (first_slot + 1 + position // node_count % (node_count - 1)) % node_count
    first = jnp.take(node_order, first_slot, axis=1)
    second = jnp.take(node_order, second_slot, axis=1)
    busy = jax.random.randint(keys[1], (node_count,), 0, E_NODE)
    single = jnp.take(busy, second)
    trio = jnp.stack([first * E_NODE, first * E_NODE + 1, second * E_NODE + single], axis=-1)
    shift = jax.random.randint(keys[2], (device_count, TOK_DEV, 1), 0, 3)
    column = (jnp.arange(3, dtype=jnp.int32)[None, None, :] + shift) % 3
    trio = jnp.take_along_axis(trio, column, axis=2)
    shuffle = jax.vmap(lambda item: jax.random.permutation(item, TOK_DEV))(jax.random.split(keys[3], device_count))
    trio = jnp.take_along_axis(trio, shuffle[:, :, None], axis=1)
    return trio.reshape(TOKENS, 3).astype(jnp.int32)


def shard_levels(stream_key, extent, shards, least, top_value):
    loudness, own = 1.0, jax.random.fold_in(stream_key, 6)
    for dim, blocks in shards:
        heights = jnp.exp(jax.random.uniform(jax.random.fold_in(own, dim), (blocks,), jnp.float32, least / len(shards), top_value / len(shards)))
        loudness = loudness * jnp.repeat(heights, extent[dim] // blocks).reshape([-1 if axis == dim else 1 for axis in range(len(extent))])
    return loudness


def bell_draw(own_key, extent, deviation, bound, shards=(), kind=jnp.bfloat16):
    factor_of = shard_levels(own_key, extent, shards, -0.22, 0.18) if shards else 1.0
    array = jax.random.normal(own_key, extent, jnp.float32) * deviation * factor_of
    return jnp.minimum(jnp.maximum(array, -bound), bound).astype(kind)


def setup_inputs(seed: int = 0) -> dict:
    key_of = jax.random.split(jax.random.key(seed), 11)
    tokens = bell_draw(key_of[0], (TOKENS, D), 1.0, 6.0, ((0, 128),))
    grad_out = bell_draw(key_of[1], (TOKENS, D), 1.0, 6.0, ((0, 128),))
    gates = jnp.clip(0.19921875 + 0.80078125 * jax.random.uniform(key_of[2], (TOKENS, TOPK), jnp.float32) ** shard_levels(key_of[2], (TOKENS, TOPK), ((0, 128),), -0.2, 0.2), 0.19921875, 1.0).astype(jnp.bfloat16)
    expert_ids = draw_expert_ids(jax.random.fold_in(key_of[10], 71), 0)
    w_gate = bell_draw(key_of[4], (N_NODE, D, E_NODE * FF), D ** -0.5, 0.0625, ((0, 8), (2, 16)))
    w_up = bell_draw(key_of[5], (N_NODE, D, E_NODE * FF), D ** -0.5, 0.0625, ((0, 8), (2, 16)))
    w_down = bell_draw(key_of[6], (N_NODE, D, E_NODE * FF), FF ** -0.5, 0.1875, ((0, 8), (2, 16)))
    s_gate = bell_draw(key_of[7], (D, FFS), D ** -0.5, 0.0625, ((1, 16),))
    s_up = bell_draw(key_of[8], (D, FFS), D ** -0.5, 0.0625, ((1, 16),))
    s_down = bell_draw(key_of[9], (D, FFS), FFS ** -0.5, 0.125, ((1, 16),))
    return {"tokens": tokens, "grad_out": grad_out, "gates": gates, "expert_ids": expert_ids, "w_gate": w_gate, "w_up": w_up, "w_down": w_down, "s_gate": s_gate, "s_up": s_up, "s_down": s_down}


def silu_parts(pre_gate):
    sig = jax.nn.sigmoid(pre_gate)
    return pre_gate * sig, sig * (1.0 + pre_gate * (1.0 - sig))


def contract_first(left, right):
    return lax.dot_general(left, right, (((0,), (0,)), ((), ())), preferred_element_type=jnp.float32)


def contract_last(left, right):
    return lax.dot_general(left, right, (((1,), (1,)), ((), ())), preferred_element_type=jnp.float32)


def ffn_backward(rows_in, rows_grad, weight, gate_w, up_w, down_w):
    pre_gate = jnp.dot(rows_in, gate_w, preferred_element_type=jnp.float32)
    pre_up = jnp.dot(rows_in, up_w, preferred_element_type=jnp.float32)
    activ, slope = silu_parts(pre_gate)
    hidden = activ * pre_up
    upstream = jnp.dot(rows_grad, down_w, preferred_element_type=jnp.float32)
    scaled = weight * upstream
    grad_up = (scaled * activ).astype(jnp.bfloat16)
    grad_gate = (scaled * pre_up * slope).astype(jnp.bfloat16)
    weighted = (weight * hidden).astype(jnp.bfloat16)
    return grad_gate, grad_up, weighted, hidden * upstream


def block_rows(grad_gate, grad_up, gate_w, up_w, width):
    blocks = gate_w.shape[1] // width

    def step(index, total):
        start = index * width
        part = contract_last(lax.dynamic_slice_in_dim(grad_gate, start, width, 1), lax.dynamic_slice_in_dim(gate_w, start, width, 1))
        part = part + contract_last(lax.dynamic_slice_in_dim(grad_up, start, width, 1), lax.dynamic_slice_in_dim(up_w, start, width, 1))
        rounded = lax.optimization_barrier(part.astype(jnp.bfloat16))
        return total + rounded.astype(jnp.float32)

    return lax.fori_loop(0, blocks, step, jnp.zeros((grad_gate.shape[0], gate_w.shape[0]), jnp.float32))


def block_stat(product, width):
    sums = jnp.sum(product.reshape(product.shape[0], -1, width), axis=2)
    return jnp.sum(lax.optimization_barrier(sums.astype(jnp.bfloat16)).astype(jnp.float32), axis=1)


def reference(tokens, grad_out, gates, expert_ids, w_gate, w_up, w_down, s_gate, s_up, s_down):
    n_tok = tokens.shape[0]
    width = tokens.shape[1]
    device_count = n_tok // TOK_DEV
    slots = device_count * (2 * TOK_DEV // N_NODE)
    group_size = N_LOCAL // E_NODE
    ff_block = FF // group_size
    gate_all = gates.astype(jnp.float32)
    positions = jnp.arange(n_tok, dtype=jnp.int32)

    def per_expert(carry, expert):
        dx_acc, dgate_acc = carry
        chosen = expert_ids == expert
        member = jnp.any(chosen, axis=1)
        weight = jnp.sum(jnp.where(chosen, gate_all, 0.0), axis=1)
        ranking = jnp.cumsum(member.astype(jnp.int32)) - 1
        target = jnp.where(member, ranking, slots).astype(jnp.int32)
        index = jnp.zeros((slots + 1,), jnp.int32).at[target].set(positions)[:slots]
        valid = jnp.zeros((slots + 1,), jnp.float32).at[target].set(1.0)[:slots]
        rows_in = tokens[index]
        rows_grad = grad_out[index]
        row_weight = (weight[index] * valid)[:, None]
        node = expert // E_NODE
        column = (expert % E_NODE) * FF
        gate_w = lax.dynamic_slice_in_dim(lax.dynamic_index_in_dim(w_gate, node, 0, keepdims=False), column, FF, 1)
        up_w = lax.dynamic_slice_in_dim(lax.dynamic_index_in_dim(w_up, node, 0, keepdims=False), column, FF, 1)
        down_w = lax.dynamic_slice_in_dim(lax.dynamic_index_in_dim(w_down, node, 0, keepdims=False), column, FF, 1)
        grad_gate, grad_up, weighted, product = ffn_backward(rows_in, rows_grad, row_weight, gate_w, up_w, down_w)
        partial_value = block_rows(grad_gate, grad_up, gate_w, up_w, ff_block)
        stat = block_stat(product, ff_block)
        dx_acc = dx_acc.at[index].add(partial_value * valid[:, None])
        token_stat = jnp.zeros((n_tok,), jnp.float32).at[index].add(stat * valid)
        dgate_acc = dgate_acc + jnp.where(chosen, token_stat[:, None], 0.0)
        grads = (contract_first(rows_in, grad_gate).astype(jnp.bfloat16), contract_first(rows_in, grad_up).astype(jnp.bfloat16), contract_first(rows_grad, weighted).astype(jnp.bfloat16))
        return (dx_acc, dgate_acc), grads

    start_carry = (jnp.zeros((n_tok, width), jnp.float32), jnp.zeros(expert_ids.shape, jnp.float32))
    (dx_routed, dgates), stacked = lax.scan(per_expert, start_carry, jnp.arange(E_NODE * N_NODE, dtype=jnp.int32))

    def arrange(grad):
        shaped = grad.reshape(N_NODE, E_NODE, width, FF)
        return jnp.transpose(shaped, (0, 2, 1, 3)).reshape(N_NODE, width, E_NODE * FF)

    unit_weight = jnp.ones((n_tok, 1), jnp.float32)
    grad_gate, grad_up, weighted, product = ffn_backward(tokens, grad_out, unit_weight, s_gate, s_up, s_down)
    dx_shared = block_rows(grad_gate, grad_up, s_gate, s_up, FFS // N_LOCAL)
    per_node = n_tok // N_NODE

    def node_step(index, totals):
        start = index * per_node
        rows_in = lax.dynamic_slice_in_dim(tokens, start, per_node, 0)
        rows_grad = lax.dynamic_slice_in_dim(grad_out, start, per_node, 0)
        parts = (contract_first(rows_in, lax.dynamic_slice_in_dim(grad_gate, start, per_node, 0)), contract_first(rows_in, lax.dynamic_slice_in_dim(grad_up, start, per_node, 0)), contract_first(rows_grad, lax.dynamic_slice_in_dim(weighted, start, per_node, 0)))
        return tuple(total + lax.optimization_barrier(part.astype(jnp.bfloat16)).astype(jnp.float32) for total, part in zip(totals, parts))

    empty = jnp.zeros((width, FFS), jnp.float32)
    shared = lax.fori_loop(0, N_NODE, node_step, (empty, empty, empty))
    dx = (dx_routed + dx_shared).astype(jnp.bfloat16)
    return (dx, dgates, arrange(stacked[0]), arrange(stacked[1]), arrange(stacked[2]), shared[0].astype(jnp.bfloat16), shared[1].astype(jnp.bfloat16), shared[2].astype(jnp.bfloat16))
```

```python
import jax
import jax.numpy as jnp
from jax import lax
from jax.sharding import Mesh, PartitionSpec as P

E_NODE = 2
RING = 4
LANES = 128
BF16 = jnp.bfloat16
F32 = jnp.float32


def shift(value, axis, by):
    return lax.ppermute(value, axis, [(i, (i + by) % RING) for i in range(RING)])


def ring_gather(value, axis):
    half = value.shape[0] // 2
    before = shift(value, axis, 1)
    after = shift(value, axis, -1)
    far = [shift(before[:half], axis, 1), shift(after[half:], axis, -1)]
    return [[value], [before], far, [after]]


def ring_scatter(blocks, axis):
    half = blocks[0].shape[0] // 2
    rest = [(0, 0)] * (blocks[0].ndim - 1)

    def total(*terms):
        return sum(t.astype(F32) for t in terms).astype(BF16)

    far_down = shift(blocks[2][:half], axis, -1)
    far_up = shift(blocks[2][half:], axis, 1)
    down = shift(total(blocks[1], jnp.pad(far_down, [(0, half)] + rest)), axis, -1)
    up = shift(total(blocks[3], jnp.pad(far_up, [(half, 0)] + rest)), axis, 1)
    return total(blocks[0], down, up)


def plane_gather(tokens, grads):
    rows = tokens.shape[0]
    along_x = jnp.concatenate(sum(ring_gather(tokens, "x"), []), axis=0)
    all_tokens = jnp.concatenate(sum(ring_gather(along_x, "y"), []), axis=0)
    along_y = jnp.concatenate(sum(ring_gather(grads, "y"), []), axis=0)
    columns = [jnp.concatenate(c, axis=0) for c in ring_gather(along_y, "x")]
    all_grads = jnp.concatenate(
        [columns[kx][ky * rows : (ky + 1) * rows] for ky in range(RING) for kx in range(RING)],
        axis=0,
    )
    return all_tokens, all_grads


def plane_scatter(left, right):
    rows = left.shape[0] // (RING * RING)

    def both(value, first, second):
        part = value.reshape(RING, RING * rows, -1)
        part = ring_scatter([part[k] for k in range(RING)], first).reshape(RING, rows, -1)
        return ring_scatter([part[k] for k in range(RING)], second)

    return jnp.concatenate([both(left, "y", "x"), both(right, "x", "y")], axis=1)


def silu_parts(pre_gate):
    sig = jax.nn.sigmoid(pre_gate)
    return (pre_gate * sig, sig * (1.0 + pre_gate * (1.0 - sig)))


def contract_first(left, right):
    return lax.dot_general(
        left, right, (((0,), (0,)), ((), ())), preferred_element_type=F32
    )


def contract_last(left, right):
    return lax.dot_general(
        left, right, (((1,), (1,)), ((), ())), preferred_element_type=F32
    )


def ffn_backward(rows_in, rows_grad, weight, gate_up, down):
    units = down.shape[1]
    both = jnp.dot(rows_in, gate_up, preferred_element_type=F32)
    upstream = jnp.dot(rows_grad, down, preferred_element_type=F32)
    pre_gate, pre_up = both[:, :units], both[:, units:]
    activ, slope = silu_parts(pre_gate)
    hidden = activ * pre_up
    scaled = upstream if weight is None else weight * upstream
    grad_up = (scaled * activ).astype(BF16)
    grad_gate = (scaled * pre_up * slope).astype(BF16)
    weighted = (hidden if weight is None else weight * hidden).astype(BF16)
    return jnp.concatenate([grad_gate, grad_up], axis=1), weighted, hidden * upstream


def turn(value):
    rows = value.shape[0] // (RING * RING)
    return value.reshape(RING, RING, rows, -1).swapaxes(0, 1).reshape(value.shape)


def local(tokens, grad_out, gates, expert_ids, w_gate, w_up, w_down, s_gate, s_up, s_down):
    here, width = tokens.shape
    units = s_gate.shape[1]
    nodes = 8
    slots_of = 2 * here // nodes
    node_axes = ("z", "core")
    split = (width // LANES + 1) // 2 * LANES

    position = lax.axis_index("y") * RING + lax.axis_index("x")
    upper = position >= (RING * RING) // E_NODE
    node_ids = jnp.arange(nodes, dtype=jnp.int32)
    chosen_node = (expert_ids[:, :, None] // E_NODE) == node_ids[None, None, :]
    member = jnp.any(chosen_node, axis=1)
    earlier = jnp.tril(jnp.ones((here, here), F32), -1)
    ranking = jnp.dot(earlier, member.astype(F32), preferred_element_type=F32)
    slots = jnp.arange(slots_of, dtype=F32)
    pick = member[:, :, None] & (ranking[:, :, None] == slots[None, None, :])
    pick = pick.reshape(here, nodes * slots_of).astype(BF16)
    expert_of = jnp.arange(E_NODE, dtype=jnp.int32)
    gate_of = jnp.where(
        expert_ids[:, :, None, None] == node_ids[:, None] * E_NODE + expert_of,
        gates.astype(F32)[:, :, None, None],
        0.0,
    ).sum(axis=1)
    slot_gate = (
        pick.astype(F32).reshape(here, nodes, slots_of, 1) * gate_of[:, :, None, :]
    ).sum(axis=0)
    slot_gate = slot_gate.reshape(nodes * slots_of, E_NODE).astype(BF16)
    send = jnp.concatenate(
        [
            contract_first(pick, tokens).astype(BF16),
            jnp.pad(slot_gate, ((0, 0), (0, LANES - E_NODE))),
            contract_first(pick, grad_out).astype(BF16),
        ],
        axis=1,
    )
    got = lax.all_to_all(
        send.reshape(nodes, slots_of, -1), node_axes, split_axis=0, concat_axis=0, tiled=True
    )
    got = got.reshape(nodes * slots_of, -1)

    shared_gate_up = jnp.concatenate([s_gate, s_up], axis=1)
    shared = lax.all_gather(
        jnp.concatenate([tokens, grad_out], axis=1), ("y", "x"), axis=0, tiled=True
    )
    shared_in, shared_grad = shared[:, :width], shared[:, width:]
    g_shared, h_shared, _ = ffn_backward(shared_in, shared_grad, None, shared_gate_up, s_down)
    dx_shared = lax.psum_scatter(
        contract_last(g_shared, shared_gate_up).astype(BF16),
        ("y", "x"),
        scatter_dimension=0,
        tiled=True,
    )
    shares = lax.psum_scatter(
        jnp.concatenate(
            [contract_first(shared_in, g_shared), contract_first(shared_grad, h_shared)], axis=1
        ).astype(BF16),
        node_axes,
        scatter_dimension=0,
        tiled=True,
    )

    gate_up = jnp.concatenate([w_gate[0], w_up[0]], axis=1)
    down = w_down[0]
    mine = jnp.arange(LANES, dtype=jnp.int32)[None, :] == position
    rows_in, rows_grad = plane_gather(got[:, : width + LANES], got[:, width + LANES :])
    pair = rows_in[:, width : width + E_NODE].astype(F32)
    weight = jnp.where(upper, pair[:, 1:2], pair[:, 0:1])
    rows_in = rows_in[:, :width]
    g, h, product = ffn_backward(rows_in, rows_grad, weight, gate_up, down)
    score = jnp.sum(product, axis=1, keepdims=True)
    score = jnp.where(mine, turn(score), 0.0).astype(BF16)
    left = contract_last(g, gate_up[:split]).astype(BF16)
    right = contract_last(turn(g), gate_up[split:]).astype(BF16)
    slot_dx = plane_scatter(left, jnp.concatenate([right, score], axis=1))
    grads = (
        contract_first(rows_in, g[:, :units]),
        contract_first(rows_in, g[:, units:]),
        contract_first(rows_grad, h),
    )

    back = lax.all_to_all(
        slot_dx.reshape(nodes, slots_of, -1),
        node_axes,
        split_axis=0,
        concat_axis=0,
        tiled=True,
    ).reshape(nodes * slots_of, -1)
    dx = jnp.dot(pick, back[:, :width], preferred_element_type=F32) + dx_shared.astype(F32)
    group = (RING * RING) // E_NODE
    slot_score = back[:, width : width + RING * RING].astype(F32)
    slot_score = slot_score.reshape(nodes, slots_of, E_NODE, group).sum(axis=3)
    token_score = (
        pick.astype(F32).reshape(here, nodes, slots_of, 1) * slot_score[None]
    ).sum(axis=2)
    token_score = token_score.reshape(here, 1, nodes * E_NODE)
    experts = jnp.arange(nodes * E_NODE, dtype=jnp.int32)
    chosen = expert_ids[:, :, None] == experts[None, None, :]
    dgates = jnp.sum(jnp.where(chosen, token_score, 0.0), axis=2)
    return (
        dx.astype(BF16),
        dgates,
        grads[0].astype(BF16)[None],
        grads[1].astype(BF16)[None],
        grads[2].astype(BF16)[None],
        shares[:, :units],
        shares[:, units : 2 * units],
        shares[:, 2 * units :],
    )


def solution(mesh):
    grid = Mesh(mesh.devices.reshape(4, 2, 4, 4), ("z", "core", "y", "x"))
    node, place = ("z", "core"), ("y", "x")
    rows = P(node + place, None)
    routed = P(node, None, place)
    return jax.shard_map(
        local,
        mesh=grid,
        in_specs=(rows,) * 4 + (routed,) * 3 + (P(None, place),) * 3,
        out_specs=(rows, rows, routed, routed, routed) + (P(node, place),) * 3,
        check_vma=False,
    )
```
